8 devices in a mesh: dp: 2 (over z, y), tp: 4 (over x, core).
Axes of the slice: x: 2, y: 2, z: 1, core: 2. Of those that a mesh axis runs over, the one named last changes fastest.
Arguments:
- x_seq: bfloat16 [4, 1024, 8192], P('dp', 'tp'), parts along dimension 0
- ln_gain: bfloat16 [8192], replicated
- w_qkv: bfloat16 [8192, 8, 1280], P(None, 'tp')
- w_out: bfloat16 [8192, 8192], P('tp')
- y_grad: bfloat16 [4, 1024, 8192], P('dp', 'tp'), parts along dimension 0
Outputs:
- output 1: bfloat16 [4, 1024, 8192], P('dp', 'tp'), parts along dimension 0
- output 2: bfloat16 [4, 1024, 8192], P('dp', 'tp'), parts along dimension 0
- output 3: bfloat16 [16384], P('dp'), parts along dimension 0
- output 4: bfloat16 [16384, 8, 1280], P('dp', 'tp'), parts along dimension 0
- output 5: bfloat16 [16384, 8192], P(('dp', 'tp')), parts along dimension 0
There are 2 independent parts. The reference program is written for one: setup_inputs(seed, part) draws one part's arguments, and reference() takes and returns one part's arrays. A program takes and returns all parts, laid end to end along the dimension named above; an argument that names none is the same for every part.
All inputs are finite; a program needn't handle non-finite values.
Results may differ from the reference program's by a relative error of at most 0.0165068.
Values are sent between devices in bfloat16 or wider.
A program may use at most 1 GiB of HBM per device.

```python
import jax
import jax.numpy as jnp
from jax import lax

BATCH_SIZE = 2
SEQ_LEN = 1024
D_MODEL = 8192
N_HEADS = 64
KV_HEADS = 8
HEAD_DIM = 128
CLIP_QKV = 8
ROPE_THETA = 500000
LN_EPS = 1e-5
GROUP_SIZE = N_HEADS // KV_HEADS
SLOT_WIDTH = (GROUP_SIZE + 2) * HEAD_DIM
OUT_GAIN = max(1.0, SEQ_LEN / 256.0) ** 0.25


def setup_inputs(seed: int = 0, part: int = 0) -> dict:
    root_key = jax.random.key(seed)
    k_gain, k_qkv, k_out = jax.random.split(root_key, 3)
    k_x, k_dy = jax.random.split(jax.random.fold_in(root_key, part), 2)
    x_seq = jax.random.normal(k_x, (BATCH_SIZE, SEQ_LEN, D_MODEL), jnp.float32)
    ln_gain = 1.0 + 0.3 * jax.random.normal(k_gain, (D_MODEL,), jnp.float32)
    slot_gain = jnp.concatenate([jnp.full((GROUP_SIZE,), 5.0, dtype=jnp.float32), jnp.array([0.35, 5.0], dtype=jnp.float32)])
    w_qkv = jax.random.normal(k_qkv, (D_MODEL, KV_HEADS, GROUP_SIZE + 2, HEAD_DIM), jnp.float32)
    w_qkv = w_qkv * slot_gain[:, None] * D_MODEL ** -0.5
    attn_width = N_HEADS * HEAD_DIM
    w_out = jax.random.normal(k_out, (attn_width, D_MODEL), jnp.float32) * (OUT_GAIN * attn_width ** -0.5)
    y_grad = jax.random.normal(k_dy, (BATCH_SIZE, SEQ_LEN, D_MODEL), jnp.float32)
    return {'x_seq': x_seq.astype(jnp.bfloat16), 'ln_gain': ln_gain.astype(jnp.bfloat16), 'w_qkv': w_qkv.reshape(D_MODEL, KV_HEADS, SLOT_WIDTH).astype(jnp.bfloat16), 'w_out': w_out.astype(jnp.bfloat16), 'y_grad': y_grad.astype(jnp.bfloat16)}


def rope_tables(seq_len):
    inv_freq = 1.0 / (ROPE_THETA ** (jnp.arange(0, HEAD_DIM, 2, dtype=jnp.float32) / HEAD_DIM))
    angles = jnp.arange(seq_len, dtype=jnp.float32)[:, None] * inv_freq[None, :]
    return jnp.cos(angles), jnp.sin(angles)


def rotate(vec_in, cos_t, sin_t):
    half_dim = vec_in.shape[-1] // 2
    half_lo = vec_in[..., :half_dim]
    half_hi = vec_in[..., half_dim:]
    return jnp.concatenate([half_lo * cos_t - half_hi * sin_t, half_hi * cos_t + half_lo * sin_t], axis=-1)


def group_attention(operands):
    query_rot, key_rot, val_head = operands
    scores = jnp.einsum('bqgd,bkd->bgqk', query_rot.astype(jnp.float32), key_rot.astype(jnp.float32)) * HEAD_DIM ** -0.5
    causal = jnp.arange(SEQ_LEN)[:, None] >= jnp.arange(SEQ_LEN)[None, :]
    scores = jnp.where(causal, scores, -1e30)
    attn_prob = jax.nn.softmax(scores, axis=-1).astype(jnp.bfloat16)
    return jnp.einsum('bgqk,bkd->bqgd', attn_prob.astype(jnp.float32), val_head.astype(jnp.float32)).astype(jnp.bfloat16)


def layer_forward(x_seq, ln_gain, w_qkv, w_out):
    x_f32 = x_seq.astype(jnp.float32)
    row_mean = jnp.mean(x_f32, axis=-1, keepdims=True)
    centered = x_f32 - row_mean
    variance = jnp.mean(centered * centered, axis=-1, keepdims=True)
    h_norm = (centered * lax.rsqrt(variance + LN_EPS) * ln_gain.astype(jnp.float32)).astype(jnp.bfloat16)
    qkv_raw = jnp.dot(h_norm.reshape(-1, D_MODEL).astype(jnp.float32), w_qkv.reshape(D_MODEL, -1).astype(jnp.float32)).astype(jnp.bfloat16)
    qkv_clip = jnp.where(jnp.abs(qkv_raw) < CLIP_QKV, qkv_raw, jnp.sign(qkv_raw) * CLIP_QKV)
    qkv_slots = qkv_clip.reshape(BATCH_SIZE, SEQ_LEN, KV_HEADS, GROUP_SIZE + 2, HEAD_DIM)
    cos_t, sin_t = rope_tables(SEQ_LEN)
    query_rot = rotate(qkv_slots[:, :, :, :GROUP_SIZE].astype(jnp.float32), cos_t[:, None, None], sin_t[:, None, None]).astype(jnp.bfloat16)
    key_rot = rotate(qkv_slots[:, :, :, GROUP_SIZE].astype(jnp.float32), cos_t[:, None], sin_t[:, None]).astype(jnp.bfloat16)
    val_head = qkv_slots[:, :, :, GROUP_SIZE + 1]
    mixed = lax.map(jax.checkpoint(group_attention), (jnp.moveaxis(query_rot, 2, 0), jnp.moveaxis(key_rot, 2, 0), jnp.moveaxis(val_head, 2, 0)))
    mixed = jnp.moveaxis(mixed, 0, 2).reshape(BATCH_SIZE * SEQ_LEN, N_HEADS * HEAD_DIM)
    out_proj = jnp.dot(mixed.astype(jnp.float32), w_out.astype(jnp.float32)).reshape(BATCH_SIZE, SEQ_LEN, D_MODEL)
    return (x_f32 + out_proj).astype(jnp.bfloat16)


def reference(x_seq, ln_gain, w_qkv, w_out, y_grad):
    y_out, pullback = jax.vjp(layer_forward, x_seq, ln_gain, w_qkv, w_out)
    x_grad, gain_grad, wqkv_grad, wout_grad = pullback(y_grad)
    return (y_out, x_grad, gain_grad, wqkv_grad, wout_grad)
```

```python
import functools
import jax
import jax.numpy as jnp
from jax import lax
from jax.experimental import pallas as pl
from jax.experimental.pallas import tpu as pltpu
from jax.sharding import PartitionSpec as P

CLIP_QKV = 8.0
ROPE_THETA = 500000.0
LN_EPS = 1e-5
LOG2E = 1.4426950408889634
QBLK = 256
NT = (((1,), (1,)), ((), ()))
NN = (((1,), (0,)), ((), ()))


def dot32(a, b, dims):
    return lax.dot_general(a, b, dims, preferred_element_type=jnp.float32)


def ln_stats(x):
    row_mean = jnp.mean(x, axis=-1, keepdims=True)
    centered = x - row_mean
    variance = jnp.mean(centered * centered, axis=-1, keepdims=True)
    rstd = lax.rsqrt(variance + LN_EPS)
    return centered * rstd, rstd


def ln_fwd_kernel(x_ref, gain_ref, h_ref):
    normed, _ = ln_stats(x_ref[0].astype(jnp.float32))
    h_ref[...] = (normed * gain_ref[...].astype(jnp.float32)).astype(jnp.bfloat16)


def ln_bwd_kernel(dh_ref, x_ref, dy_ref, gain_ref, *refs):
    dx_ref, dgain_ref = refs[-2:]
    normed, rstd = ln_stats(x_ref[0].astype(jnp.float32))
    d_h = dh_ref[...].astype(jnp.float32)
    d_gain = jnp.sum(d_h * normed, axis=0, keepdims=True)
    d_normed = d_h * gain_ref[...].astype(jnp.float32)
    shift = jnp.mean(d_normed, axis=-1, keepdims=True)
    slope = jnp.mean(d_normed * normed, axis=-1, keepdims=True)
    d_x = rstd * (d_normed - shift - normed * slope)
    dx_ref[0] = (dy_ref[0].astype(jnp.float32) + d_x).astype(jnp.bfloat16)

    @pl.when(pl.program_id(0) == 0)
    def _():
        dgain_ref[...] = d_gain

    @pl.when(pl.program_id(0) > 0)
    def _():
        dgain_ref[...] += d_gain


def residual_kernel(o_ref, x_ref, *refs):
    y_ref = refs[-1]
    y_ref[0] = (x_ref[0].astype(jnp.float32) + o_ref[...].astype(jnp.float32)).astype(jnp.bfloat16)


def interleave_kernel(in_ref, out_ref):
    for n in range(in_ref.shape[0]):
        out_ref[:, n, :] = in_ref[n]


def rope_tables(seq_len, head_dim):
    inv_freq = 1.0 / (ROPE_THETA ** (jnp.arange(0, head_dim, 2, dtype=jnp.float32) / head_dim))
    angles = jnp.arange(seq_len, dtype=jnp.float32)[:, None] * inv_freq[None, :]
    cos_t, sin_t = jnp.cos(angles), jnp.sin(angles)
    return jnp.concatenate([cos_t, cos_t], axis=-1), jnp.concatenate([-sin_t, sin_t], axis=-1)


def clip(v):
    return jnp.minimum(jnp.maximum(v, -CLIP_QKV), CLIP_QKV)


def rope(v_f32, cos_t, sin_t):
    return v_f32 * cos_t + pltpu.roll(v_f32, v_f32.shape[-1] // 2, 1) * sin_t


def unrope(v_f32, cos_t, sin_t):
    return v_f32 * cos_t - pltpu.roll(v_f32, v_f32.shape[-1] // 2, 1) * sin_t


def masked_tail(s, fill):
    top, tail = s[:-QBLK], s[-QBLK:]
    rows = lax.broadcasted_iota(jnp.int32, tail.shape, 0)
    cols = lax.broadcasted_iota(jnp.int32, tail.shape, 1)
    tail = jnp.where(rows <= cols, tail, fill)
    return tail if s.shape[0] == QBLK else jnp.concatenate([top, tail], axis=0)


def attn_fwd_kernel(groups, dim, qkv_ref, cos_ref, sin_ref, out_ref, lse_ref, k_scr, vt_scr):
    head = pl.program_id(1)
    seq = qkv_ref.shape[1]

    @pl.when(head == 0)
    def _():
        k_in = clip(qkv_ref[0, :, groups * dim:(groups + 1) * dim].astype(jnp.float32))
        k_scr[...] = rope(k_in, cos_ref[...], sin_ref[...]).astype(jnp.bfloat16)
        v_in = clip(qkv_ref[0, :, (groups + 1) * dim:(groups + 2) * dim].astype(jnp.float32))
        vt_scr[...] = v_in.T.astype(jnp.bfloat16)

    col = pl.ds(pl.multiple_of(head * dim, dim), dim)
    scale = LOG2E * dim ** -0.5
    for i in range(seq // QBLK):
        rows = slice(i * QBLK, (i + 1) * QBLK)
        kend = (i + 1) * QBLK
        q_in = clip(qkv_ref[0, rows, col].astype(jnp.float32))
        q_rot = rope(q_in, cos_ref[rows, :], sin_ref[rows, :]).astype(jnp.bfloat16)
        s = dot32(k_scr[:kend, :], q_rot, NT) * scale
        s = masked_tail(s, -1e30)
        top = jnp.max(s, axis=0, keepdims=True)
        e = jnp.exp2(s - top)
        total = jnp.sum(e, axis=0, keepdims=True)
        prob = (e * (1.0 / total)).astype(jnp.bfloat16)
        o_t = dot32(vt_scr[:, :kend], prob, NN)
        out_ref[rows, col] = o_t.T.astype(jnp.bfloat16)
        lse_ref[0, pl.ds(head, 1), rows] = top + jnp.log2(total)


def attn_bwd_kernel(groups, dim, qkv_ref, do_ref, lse_ref, cos_ref, sin_ref, dqkv_ref,
                    k_scr, kt_scr, v_scr, dk_scr, dv_scr):
    head = pl.program_id(1)
    seq = qkv_ref.shape[1]
    kcol = slice(groups * dim, (groups + 1) * dim)
    vcol = slice((groups + 1) * dim, (groups + 2) * dim)

    @pl.when(head == 0)
    def _():
        k_in = clip(qkv_ref[0, :, kcol].astype(jnp.float32))
        k_rot = rope(k_in, cos_ref[...], sin_ref[...])
        k_scr[...] = k_rot.astype(jnp.bfloat16)
        kt_scr[...] = k_rot.T.astype(jnp.bfloat16)
        v_scr[...] = clip(qkv_ref[0, :, vcol].astype(jnp.float32)).astype(jnp.bfloat16)
        dk_scr[...] = jnp.zeros_like(dk_scr)
        dv_scr[...] = jnp.zeros_like(dv_scr)

    col = pl.ds(pl.multiple_of(head * dim, dim), dim)
    scale = dim ** -0.5
    for i in range(seq // QBLK):
        rows = slice(i * QBLK, (i + 1) * QBLK)
        kend = (i + 1) * QBLK
        q_raw = qkv_ref[0, rows, col].astype(jnp.float32)
        q_rot = rope(clip(q_raw), cos_ref[rows, :], sin_ref[rows, :]).astype(jnp.bfloat16)
        d_o = do_ref[rows, col]
        s = dot32(k_scr[:kend, :], q_rot, NT) * (LOG2E * scale) - lse_ref[0, pl.ds(head, 1), rows]
        p = jnp.exp2(masked_tail(s, -1e30))
        dv_scr[:kend, :] += dot32(p.astype(jnp.bfloat16), d_o, NN)
        dp = dot32(v_scr[:kend, :], d_o, NT).astype(jnp.bfloat16).astype(jnp.float32)
        t = p * dp
        delta = jnp.sum(t, axis=0, keepdims=True)
        ds = (t - p * delta).astype(jnp.bfloat16)
        dk_scr[:kend, :] += dot32(ds, q_rot, NN)
        dq = (dot32(kt_scr[:, :kend], ds, NN) * scale).T.astype(jnp.bfloat16).astype(jnp.float32)
        dq = unrope(dq, cos_ref[rows, :], sin_ref[rows, :])
        dqkv_ref[0, rows, col] = jnp.where(jnp.abs(q_raw) < CLIP_QKV, dq, 0.0).astype(jnp.bfloat16)

    @pl.when(head == groups - 1)
    def _():
        k_raw = qkv_ref[0, :, kcol].astype(jnp.float32)
        v_raw = qkv_ref[0, :, vcol].astype(jnp.float32)
        dk = (dk_scr[...] * scale).astype(jnp.bfloat16).astype(jnp.float32)
        dk = unrope(dk, cos_ref[...], sin_ref[...])
        dqkv_ref[0, :, kcol] = jnp.where(jnp.abs(k_raw) < CLIP_QKV, dk, 0.0).astype(jnp.bfloat16)
        dqkv_ref[0, :, vcol] = jnp.where(jnp.abs(v_raw) < CLIP_QKV, dv_scr[...], 0.0).astype(jnp.bfloat16)


def attn_cost(kv_loc, groups, seq, dim, dots):
    flops = dots * 2 * kv_loc * groups * seq * seq * dim
    return pl.CostEstimate(flops=flops, bytes_accessed=2 * kv_loc * seq * dim * (2 * groups + 2) * 2,
                           transcendentals=kv_loc * groups * seq * seq // 2)


def attn_fwd(qkv, cos_t, sin_t, dim):
    kv_loc, seq, width = qkv.shape
    groups = width // dim - 2
    table = pl.BlockSpec((seq, dim), lambda n, h: (0, 0))
    return pl.pallas_call(
        functools.partial(attn_fwd_kernel, groups, dim),
        grid=(kv_loc, groups),
        in_specs=[pl.BlockSpec((1, seq, width), lambda n, h: (n, 0, 0)), table, table],
        out_specs=[pl.BlockSpec((seq, groups * dim), lambda n, h: (0, n)),
                   pl.BlockSpec((1, groups, seq), lambda n, h: (n, 0, 0))],
        out_shape=[jax.ShapeDtypeStruct((seq, kv_loc * groups * dim), jnp.bfloat16),
                   jax.ShapeDtypeStruct((kv_loc, groups, seq), jnp.float32)],
        scratch_shapes=[pltpu.VMEM((seq, dim), jnp.bfloat16), pltpu.VMEM((dim, seq), jnp.bfloat16)],
        compiler_params=pltpu.CompilerParams(dimension_semantics=("arbitrary", "arbitrary"),
                                             vmem_limit_bytes=48 * 2 ** 20),
        cost_estimate=attn_cost(kv_loc, groups, seq, dim, 4),
        name="attn_fwd",
    )(qkv, cos_t, sin_t)


def attn_bwd(qkv, d_out, lse, cos_t, sin_t, dim):
    kv_loc, seq, width = qkv.shape
    groups = width // dim - 2
    table = pl.BlockSpec((seq, dim), lambda n, h: (0, 0))
    wide = pl.BlockSpec((1, seq, width), lambda n, h: (n, 0, 0))
    return pl.pallas_call(
        functools.partial(attn_bwd_kernel, groups, dim),
        grid=(kv_loc, groups),
        in_specs=[wide, pl.BlockSpec((seq, groups * dim), lambda n, h: (0, n)),
                  pl.BlockSpec((1, groups, seq), lambda n, h: (n, 0, 0)), table, table],
        out_specs=wide,
        out_shape=jax.ShapeDtypeStruct(qkv.shape, jnp.bfloat16),
        scratch_shapes=[pltpu.VMEM((seq, dim), jnp.bfloat16), pltpu.VMEM((dim, seq), jnp.bfloat16),
                        pltpu.VMEM((seq, dim), jnp.bfloat16), pltpu.VMEM((seq, dim), jnp.float32),
                        pltpu.VMEM((seq, dim), jnp.float32)],
        compiler_params=pltpu.CompilerParams(dimension_semantics=("arbitrary", "arbitrary"),
                                             vmem_limit_bytes=48 * 2 ** 20),
        cost_estimate=attn_cost(kv_loc, groups, seq, dim, 8),
        name="attn_bwd",
    )(qkv, d_out, lse, cos_t, sin_t)


def row_call(body, rows, b, flat_in, full_in, extra_in, prev, extra_out):
    tokens, width = full_in[0].shape[1:]
    flat = pl.BlockSpec((rows, width), lambda r: (r, 0))
    full = pl.BlockSpec((1, rows, width), lambda r: (b, r, 0))
    wide = pl.BlockSpec((1, width), lambda r: (0, 0))
    args = [*flat_in, *full_in, *extra_in] + ([] if prev is None else [prev])
    specs = [flat] * len(flat_in) + [full] * len(full_in) + [wide] * len(extra_in)
    if prev is not None:
        specs.append(pl.BlockSpec(memory_space=pl.ANY))
    out_spec = flat if prev is None and not flat_in else full
    out_shape = (tokens, width) if prev is None and not flat_in else full_in[0].shape
    out_shape = [jax.ShapeDtypeStruct(out_shape, jnp.bfloat16)]
    out_shape += [jax.ShapeDtypeStruct((1, width), jnp.float32)] * extra_out
    return pl.pallas_call(
        body, grid=(tokens // rows,), in_specs=specs, out_specs=[out_spec] + [wide] * extra_out, out_shape=out_shape,
        input_output_aliases={} if prev is None else {len(args) - 1: 0},
        compiler_params=pltpu.CompilerParams(dimension_semantics=("arbitrary",), vmem_limit_bytes=40 * 2 ** 20),
        cost_estimate=pl.CostEstimate(flops=40 * tokens * width, bytes_accessed=2 * len(args) * tokens * width,
                                      transcendentals=0),
    )(*args)


def interleave(grad):
    kv_loc, rows, width = grad.shape
    block = 256
    return pl.pallas_call(
        interleave_kernel, grid=(rows // block,),
        in_specs=[pl.BlockSpec((kv_loc, block, width), lambda r: (0, r, 0))],
        out_specs=pl.BlockSpec((block, kv_loc, width), lambda r: (r, 0, 0)),
        out_shape=jax.ShapeDtypeStruct((rows, kv_loc, width), jnp.bfloat16),
        compiler_params=pltpu.CompilerParams(dimension_semantics=("arbitrary",)),
        cost_estimate=pl.CostEstimate(flops=64 * grad.size, bytes_accessed=4 * grad.size, transcendentals=0),
        name="interleave",
    )(grad)


def ein(spec, a, b):
    return jnp.einsum(spec, a, b, preferred_element_type=jnp.float32).astype(jnp.bfloat16)


def solution(mesh):
    def device_step(x_seq, ln_gain, w_qkv, w_out, y_grad):
        batch = x_seq.shape[0]
        kv_loc = w_qkv.shape[1]
        dim = (w_qkv.shape[2] - w_out.shape[0] // kv_loc) // 2
        gain = ln_gain.reshape(1, -1)
        cos_t, sin_t = rope_tables(x_seq.shape[1] * lax.axis_size('tp'), dim)

        def gather(v):
            return lax.all_gather(v, 'tp', axis=0, tiled=True)

        def scatter(v):
            return lax.psum_scatter(v, 'tp', scatter_dimension=0, tiled=True)

        h_full, g_full, qkv, attn, lse, d_qkv, outs, dhs = [], [], [], [], [], [], [], []
        for b in range(batch):
            (h_loc,) = row_call(ln_fwd_kernel, 32, b, [], [x_seq], [gain], None, 0)
            h_full.append(gather(h_loc))
        for b in range(batch):
            g_full.append(gather(y_grad[b]))
        for b in range(batch):
            qkv.append(ein('sd,dnc->nsc', h_full[b], w_qkv))
            a_b, lse_b = attn_fwd(qkv[b], cos_t, sin_t, dim)
            attn.append(a_b)
            lse.append(lse_b)
            outs.append(scatter(ein('sk,kd->sd', a_b, w_out)))
        for b in range(batch):
            d_attn = ein('sd,kd->sk', g_full[b], w_out)
            d_qkv.append(attn_bwd(qkv[b], d_attn, lse[b], cos_t, sin_t, dim))
            dhs.append(scatter(ein('nsc,dnc->sd', d_qkv[b], w_qkv)))
        h_all, g_all = jnp.concatenate(h_full, 0), jnp.concatenate(g_full, 0)
        wout_grad = ein('sk,sd->kd', jnp.concatenate(attn, 0), g_all)
        wqkv_grad = interleave(ein('sd,nsc->ndc', h_all, jnp.concatenate(d_qkv, 1)))
        y_out, x_grad, gain_part = None, None, 0.0
        for b in range(batch):
            x_grad, gain_b = row_call(ln_bwd_kernel, 32, b, [dhs[b]], [x_seq, y_grad], [gain], x_grad, 1)
            gain_part = gain_part + gain_b[0]
        gain_grad = lax.psum(gain_part, 'tp').astype(jnp.bfloat16)
        for b in range(batch):
            (y_out,) = row_call(residual_kernel, 64, b, [outs[b]], [x_seq], [], y_out, 0)
        return y_out, x_grad, gain_grad, wqkv_grad, wout_grad

    specs_in = (P('dp', 'tp', None), P(None), P(None, 'tp', None), P('tp', None), P('dp', 'tp', None))
    specs_out = (P('dp', 'tp', None), P('dp', 'tp', None), P('dp'), P('dp', 'tp', None), P(('dp', 'tp'), None))
    return jax.shard_map(device_step, mesh=mesh, in_specs=specs_in, out_specs=specs_out, check_vma=False)
```

```python
import functools
import jax
import jax.numpy as jnp
from jax import lax
from jax.experimental import pallas as pl
from jax.experimental.pallas import tpu as pltpu
from jax.sharding import PartitionSpec as P

CLIP_QKV = 8.0
ROPE_THETA = 500000.0
LN_EPS = 1e-5
LOG2E = 1.4426950408889634
QBLK = 256
NT = (((1,), (1,)), ((), ()))
NN = (((1,), (0,)), ((), ()))
TN = (((0,), (0,)), ((), ()))


def dot32(a, b, dims):
    return lax.dot_general(a, b, dims, preferred_element_type=jnp.float32)


def ln_stats(x):
    row_mean = jnp.mean(x, axis=-1, keepdims=True)
    centered = x - row_mean
    variance = jnp.mean(centered * centered, axis=-1, keepdims=True)
    rstd = lax.rsqrt(variance + LN_EPS)
    return centered * rstd, rstd


def ln_fwd_kernel(x_ref, gain_ref, h_ref):
    normed, _ = ln_stats(x_ref[0].astype(jnp.float32))
    h_ref[...] = (normed * gain_ref[...].astype(jnp.float32)).astype(jnp.bfloat16)


def ln_bwd_kernel(dh_ref, x_ref, dy_ref, gain_ref, *refs):
    dx_ref, dgain_ref = refs[-2:]
    normed, rstd = ln_stats(x_ref[0].astype(jnp.float32))
    d_h = dh_ref[...].astype(jnp.float32)
    d_gain = jnp.sum(d_h * normed, axis=0, keepdims=True)
    d_normed = d_h * gain_ref[...].astype(jnp.float32)
    shift = jnp.mean(d_normed, axis=-1, keepdims=True)
    slope = jnp.mean(d_normed * normed, axis=-1, keepdims=True)
    d_x = rstd * (d_normed - shift - normed * slope)
    dx_ref[0] = (dy_ref[0].astype(jnp.float32) + d_x).astype(jnp.bfloat16)

    @pl.when(pl.program_id(0) == 0)
    def _():
        dgain_ref[...] = d_gain

    @pl.when(pl.program_id(0) > 0)
    def _():
        dgain_ref[...] += d_gain


def residual_kernel(o_ref, x_ref, *refs):
    y_ref = refs[-1]
    y_ref[0] = (x_ref[0].astype(jnp.float32) + o_ref[...].astype(jnp.float32)).astype(jnp.bfloat16)


def rope_tables(seq_len, head_dim):
    inv_freq = 1.0 / (ROPE_THETA ** (jnp.arange(0, head_dim, 2, dtype=jnp.float32) / head_dim))
    angles = jnp.arange(seq_len, dtype=jnp.float32)[:, None] * inv_freq[None, :]
    cos_t, sin_t = jnp.cos(angles), jnp.sin(angles)
    return jnp.concatenate([cos_t, cos_t], axis=-1), jnp.concatenate([-sin_t, sin_t], axis=-1)


def clip(v):
    return jnp.minimum(jnp.maximum(v, -CLIP_QKV), CLIP_QKV)


def rope(v_f32, cos_t, sin_t):
    return v_f32 * cos_t + pltpu.roll(v_f32, v_f32.shape[-1] // 2, 1) * sin_t


def unrope(v_f32, cos_t, sin_t):
    return v_f32 * cos_t - pltpu.roll(v_f32, v_f32.shape[-1] // 2, 1) * sin_t


def masked_tail(s, fill):
    top, tail = s[:-QBLK], s[-QBLK:]
    rows = lax.broadcasted_iota(jnp.int32, tail.shape, 0)
    cols = lax.broadcasted_iota(jnp.int32, tail.shape, 1)
    tail = jnp.where(rows <= cols, tail, fill)
    return tail if s.shape[0] == QBLK else jnp.concatenate([top, tail], axis=0)


def half_rows(chip_ref, seq):
    half = seq // 2
    own = pl.multiple_of(chip_ref[0] * half, half)
    return half, pl.ds(own, half), pl.ds(half - own, half)


def join(chip_ref, own_ref, oth_ref, dst):
    _, own, oth = half_rows(chip_ref, dst.shape[0])
    dst[own, :] = own_ref[...].reshape(own_ref.shape[-2:])
    dst[oth, :] = oth_ref[...].reshape(oth_ref.shape[-2:])


def split(chip_ref, src, dst_ref):
    half, own, oth = half_rows(chip_ref, src.shape[-2])
    at = (0,) * (len(src.shape) - 2)
    dst_ref[at + (slice(0, half),)] = src[at + (own,)]
    dst_ref[at + (slice(half, 2 * half),)] = src[at + (oth,)]


def attn_fwd_kernel(groups, dim, chip_ref, own_ref, oth_ref, cos_ref, sin_ref, out_ref, perm_ref, lse_ref,
                    qkv_scr, k_scr, vt_scr):
    head = pl.program_id(1)
    seq = qkv_scr.shape[0]

    @pl.when(head == 0)
    def _():
        join(chip_ref, own_ref, oth_ref, qkv_scr)
        k_in = clip(qkv_scr[:, groups * dim:(groups + 1) * dim].astype(jnp.float32))
        k_scr[...] = rope(k_in, cos_ref[...], sin_ref[...]).astype(jnp.bfloat16)
        v_in = clip(qkv_scr[:, (groups + 1) * dim:(groups + 2) * dim].astype(jnp.float32))
        vt_scr[...] = v_in.T.astype(jnp.bfloat16)

    col = pl.ds(pl.multiple_of(head * dim, dim), dim)
    scale = LOG2E * dim ** -0.5

    def scores(i):
        rows = slice(i * QBLK, (i + 1) * QBLK)
        q_in = clip(qkv_scr[rows, col].astype(jnp.float32))
        q_rot = rope(q_in, cos_ref[rows, :], sin_ref[rows, :]).astype(jnp.bfloat16)
        return dot32(k_scr[:(i + 1) * QBLK, :], q_rot, NT)

    for i in range(seq // QBLK):
        rows = slice(i * QBLK, (i + 1) * QBLK)
        s = masked_tail(scores(i) * scale, -1e30)
        top = jnp.max(s, axis=0, keepdims=True)
        e = jnp.exp2(s - top)
        total = jnp.sum(e, axis=0, keepdims=True)
        prob = (e * (1.0 / total)).astype(jnp.bfloat16)
        o_t = dot32(vt_scr[:, :(i + 1) * QBLK], prob, NN)
        out_ref[rows, col] = o_t.T.astype(jnp.bfloat16)
        lse_ref[0, pl.ds(head, 1), rows] = top + jnp.log2(total)

    @pl.when(head == groups - 1)
    def _():
        split(chip_ref, out_ref, perm_ref)


def attn_bwd_kernel(groups, dim, chip_ref, own_ref, oth_ref, do_own_ref, do_oth_ref, lse_ref, cos_ref, sin_ref,
                    dqkv_ref, perm_ref, qkv_scr, do_scr, k_scr, kt_scr, v_scr, dk_scr, dv_scr):
    head = pl.program_id(1)
    seq = qkv_scr.shape[0]
    kcol = slice(groups * dim, (groups + 1) * dim)
    vcol = slice((groups + 1) * dim, (groups + 2) * dim)

    @pl.when(head == 0)
    def _():
        join(chip_ref, own_ref, oth_ref, qkv_scr)
        join(chip_ref, do_own_ref, do_oth_ref, do_scr)
        k_in = clip(qkv_scr[:, kcol].astype(jnp.float32))
        k_rot = rope(k_in, cos_ref[...], sin_ref[...])
        k_scr[...] = k_rot.astype(jnp.bfloat16)
        kt_scr[...] = k_rot.T.astype(jnp.bfloat16)
        v_scr[...] = clip(qkv_scr[:, vcol].astype(jnp.float32)).astype(jnp.bfloat16)
        dk_scr[...] = jnp.zeros_like(dk_scr)
        dv_scr[...] = jnp.zeros_like(dv_scr)

    col = pl.ds(pl.multiple_of(head * dim, dim), dim)
    scale = dim ** -0.5
    for i in range(seq // QBLK):
        rows = slice(i * QBLK, (i + 1) * QBLK)
        kend = (i + 1) * QBLK
        q_raw = qkv_scr[rows, col].astype(jnp.float32)
        q_rot = rope(clip(q_raw), cos_ref[rows, :], sin_ref[rows, :]).astype(jnp.bfloat16)
        d_o = do_scr[rows, col]
        s = dot32(k_scr[:kend, :], q_rot, NT) * (LOG2E * scale) - lse_ref[0, pl.ds(head, 1), rows]
        p = jnp.exp2(masked_tail(s, -1e30))
        dv_scr[:kend, :] += dot32(p.astype(jnp.bfloat16), d_o, NN)
        dp = dot32(v_scr[:kend, :], d_o, NT).astype(jnp.bfloat16).astype(jnp.float32)
        t = p * dp
        delta = jnp.sum(t, axis=0, keepdims=True)
        ds = (t - p * delta).astype(jnp.bfloat16)
        dk_scr[:kend, :] += dot32(ds, q_rot, NN)
        dq = (dot32(kt_scr[:, :kend], ds, NN) * scale).T.astype(jnp.bfloat16).astype(jnp.float32)
        dq = unrope(dq, cos_ref[rows, :], sin_ref[rows, :])
        dqkv_ref[0, rows, col] = jnp.where(jnp.abs(q_raw) < CLIP_QKV, dq, 0.0).astype(jnp.bfloat16)

    @pl.when(head == groups - 1)
    def _():
        k_raw = qkv_scr[:, kcol].astype(jnp.float32)
        v_raw = qkv_scr[:, vcol].astype(jnp.float32)
        dk = (dk_scr[...] * scale).astype(jnp.bfloat16).astype(jnp.float32)
        dk = unrope(dk, cos_ref[...], sin_ref[...])
        dqkv_ref[0, :, kcol] = jnp.where(jnp.abs(k_raw) < CLIP_QKV, dk, 0.0).astype(jnp.bfloat16)
        dqkv_ref[0, :, vcol] = jnp.where(jnp.abs(v_raw) < CLIP_QKV, dv_scr[...], 0.0).astype(jnp.bfloat16)
        split(chip_ref, dqkv_ref, perm_ref)


VMEM_MAX = 63 * 2 ** 20


def attn_params(kv_loc, groups, seq, dim, dots):
    return dict(
        compiler_params=pltpu.CompilerParams(dimension_semantics=("arbitrary", "arbitrary"),
                                             vmem_limit_bytes=VMEM_MAX),
        cost_estimate=pl.CostEstimate(flops=dots * 2 * kv_loc * groups * seq * seq * dim,
                                      bytes_accessed=2 * kv_loc * seq * dim * (2 * groups + 2) * 2,
                                      transcendentals=kv_loc * groups * seq * seq // 2))


def attn_fwd(chip, own, oth, cos_t, sin_t, dim):
    kv_loc, half, width = own.shape
    seq = 2 * half
    groups = width // dim - 2
    table = pl.BlockSpec((seq, dim), lambda n, h: (0, 0))
    piece = pl.BlockSpec((1, half, width), lambda n, h: (n, 0, 0))
    heads = pl.BlockSpec((seq, groups * dim), lambda n, h: (0, n))
    heads_shape = jax.ShapeDtypeStruct((seq, kv_loc * groups * dim), jnp.bfloat16)
    return pl.pallas_call(
        functools.partial(attn_fwd_kernel, groups, dim),
        grid=(kv_loc, groups),
        in_specs=[pl.BlockSpec(memory_space=pltpu.SMEM), piece, piece, table, table],
        out_specs=[heads, heads, pl.BlockSpec((1, groups, seq), lambda n, h: (n, 0, 0))],
        out_shape=[heads_shape, heads_shape, jax.ShapeDtypeStruct((kv_loc, groups, seq), jnp.float32)],
        scratch_shapes=[pltpu.VMEM((seq, width), jnp.bfloat16), pltpu.VMEM((seq, dim), jnp.bfloat16),
                        pltpu.VMEM((dim, seq), jnp.bfloat16)],
        name="attn_fwd",
        **attn_params(kv_loc, groups, seq, dim, 4),
    )(chip, own, oth, cos_t, sin_t)


def attn_bwd(chip, own, oth, do_own, do_oth, lse, cos_t, sin_t, dim):
    kv_loc, half, width = own.shape
    seq = 2 * half
    groups = width // dim - 2
    table = pl.BlockSpec((seq, dim), lambda n, h: (0, 0))
    piece = pl.BlockSpec((1, half, width), lambda n, h: (n, 0, 0))
    d_piece = pl.BlockSpec((half, groups * dim), lambda n, h: (0, n))
    wide = pl.BlockSpec((1, seq, width), lambda n, h: (n, 0, 0))
    wide_shape = jax.ShapeDtypeStruct((kv_loc, seq, width), jnp.bfloat16)
    return pl.pallas_call(
        functools.partial(attn_bwd_kernel, groups, dim),
        grid=(kv_loc, groups),
        in_specs=[pl.BlockSpec(memory_space=pltpu.SMEM), piece, piece, d_piece, d_piece,
                  pl.BlockSpec((1, groups, seq), lambda n, h: (n, 0, 0)), table, table],
        out_specs=[wide, wide],
        out_shape=[wide_shape, wide_shape],
        scratch_shapes=[pltpu.VMEM((seq, width), jnp.bfloat16), pltpu.VMEM((seq, groups * dim), jnp.bfloat16),
                        pltpu.VMEM((seq, dim), jnp.bfloat16), pltpu.VMEM((dim, seq), jnp.bfloat16),
                        pltpu.VMEM((seq, dim), jnp.bfloat16), pltpu.VMEM((seq, dim), jnp.float32),
                        pltpu.VMEM((seq, dim), jnp.float32)],
        name="attn_bwd",
        **attn_params(kv_loc, groups, seq, dim, 8),
    )(chip, own, oth, do_own, do_oth, lse, cos_t, sin_t)


def wqkv_grad_kernel(pieces, *refs):
    h_refs, d_refs, out_ref = refs[:pieces], refs[pieces:-1], refs[-1]
    half = h_refs[0].shape[0]
    for n in range(out_ref.shape[1]):
        total = 0.0
        for j in range(pieces):
            at = half * (j % 2)
            total += dot32(h_refs[j][...], d_refs[j // 2][n, at:at + half, :], TN)
        out_ref[:, n, :] = total.astype(jnp.bfloat16)


def wqkv_grad_call(h_pieces, d_qkv):
    half, rows = h_pieces[0].shape
    kv_loc, seq, width = d_qkv[0].shape
    block = 256
    return pl.pallas_call(
        functools.partial(wqkv_grad_kernel, len(h_pieces)), grid=(rows // block,),
        in_specs=[pl.BlockSpec((half, block), lambda r: (0, r))] * len(h_pieces)
        + [pl.BlockSpec((kv_loc, seq, width), lambda r: (0, 0, 0))] * len(d_qkv),
        out_specs=pl.BlockSpec((block, kv_loc, width), lambda r: (r, 0, 0)),
        out_shape=jax.ShapeDtypeStruct((rows, kv_loc, width), jnp.bfloat16),
        compiler_params=pltpu.CompilerParams(dimension_semantics=("arbitrary",), vmem_limit_bytes=VMEM_MAX),
        cost_estimate=pl.CostEstimate(flops=2 * half * len(h_pieces) * rows * kv_loc * width,
                                      bytes_accessed=4 * rows * kv_loc * width, transcendentals=0),
        name="wqkv_grad",
    )(*h_pieces, *d_qkv)


def row_call(body, rows, b, flat_in, full_in, extra_in, prev, extra_out):
    tokens, width = full_in[0].shape[1:]
    flat = pl.BlockSpec((rows, width), lambda r: (r, 0))
    full = pl.BlockSpec((1, rows, width), lambda r: (b, r, 0))
    wide = pl.BlockSpec((1, width), lambda r: (0, 0))
    args = [*flat_in, *full_in, *extra_in] + ([] if prev is None else [prev])
    specs = [flat] * len(flat_in) + [full] * len(full_in) + [wide] * len(extra_in)
    if prev is not None:
        specs.append(pl.BlockSpec(memory_space=pl.ANY))
    out_spec = flat if prev is None and not flat_in else full
    out_shape = (tokens, width) if prev is None and not flat_in else full_in[0].shape
    out_shape = [jax.ShapeDtypeStruct(out_shape, jnp.bfloat16)]
    out_shape += [jax.ShapeDtypeStruct((1, width), jnp.float32)] * extra_out
    return pl.pallas_call(
        body, grid=(tokens // rows,), in_specs=specs, out_specs=[out_spec] + [wide] * extra_out, out_shape=out_shape,
        input_output_aliases={} if prev is None else {len(args) - 1: 0},
        compiler_params=pltpu.CompilerParams(dimension_semantics=("arbitrary",), vmem_limit_bytes=VMEM_MAX),
        cost_estimate=pl.CostEstimate(flops=40 * tokens * width, bytes_accessed=2 * len(args) * tokens * width,
                                      transcendentals=0),
    )(*args)


def ein(spec, a, b):
    return jnp.einsum(spec, a, b, preferred_element_type=jnp.float32).astype(jnp.bfloat16)


def solution(mesh):
    def device_step(x_seq, ln_gain, w_qkv, w_out, y_grad):
        batch = x_seq.shape[0]
        kv_loc = w_qkv.shape[1]
        dim = (w_qkv.shape[2] - w_out.shape[0] // kv_loc) // 2
        gain = ln_gain.reshape(1, -1)
        cos_t, sin_t = rope_tables(x_seq.shape[1] * lax.axis_size('tp'), dim)
        chip = (lax.axis_index('tp') // 2).astype(jnp.int32).reshape(1)

        def across(v):
            return lax.ppermute(v, 'tp', [(d, (d + 2) % 4) for d in range(4)])

        def pair(v):
            return lax.all_gather(v, 'tp', axis=0, tiled=True, axis_index_groups=[[0, 1], [2, 3]])

        def scatter(v):
            return lax.psum_scatter(v, 'tp', scatter_dimension=0, tiled=True)

        seqs = range(batch)
        h_loc = [row_call(ln_fwd_kernel, 32, b, [], [x_seq], [gain], None, 0)[0] for b in seqs]
        g_loc = [y_grad[b] for b in seqs]
        h_far = [across(h_loc[b]) for b in seqs]
        g_far = [across(g_loc[b]) for b in seqs]
        h_own = [pair(h_loc[b]) for b in seqs]
        g_own = [pair(g_loc[b]) for b in seqs]
        h_oth = [pair(h_far[b]) for b in seqs]
        g_oth = [pair(g_far[b]) for b in seqs]
        qkv_own = [ein('sd,dnc->nsc', h_own[b], w_qkv) for b in seqs]
        d_own = [ein('sd,kd->sk', g_own[b], w_out) for b in seqs]
        qkv_oth, attn_perm, lse, outs, d_perm, dhs = [], [], [], [], [], []
        for b in seqs:
            qkv_oth.append(ein('sd,dnc->nsc', h_oth[b], w_qkv))
            a_seq, a_perm, lse_b = attn_fwd(chip, qkv_own[b], qkv_oth[b], cos_t, sin_t, dim)
            attn_perm.append(a_perm)
            lse.append(lse_b)
            outs.append(scatter(ein('sk,kd->sd', a_seq, w_out)))
        for b in seqs:
            d_oth = ein('sd,kd->sk', g_oth[b], w_out)
            d_seq, d_perm_b = attn_bwd(chip, qkv_own[b], qkv_oth[b], d_own[b], d_oth, lse[b], cos_t, sin_t, dim)
            d_perm.append(d_perm_b)
            dhs.append(scatter(ein('nsc,dnc->sd', d_seq, w_qkv)))
        g_all = jnp.concatenate([v for b in seqs for v in (g_own[b], g_oth[b])], 0)
        wout_grad = ein('sk,sd->kd', jnp.concatenate(attn_perm, 0), g_all)
        wqkv_grad = wqkv_grad_call([v for b in seqs for v in (h_own[b], h_oth[b])], d_perm)
        y_out, x_grad, gain_part = None, None, 0.0
        for b in seqs:
            (y_out,) = row_call(residual_kernel, 64, b, [outs[b]], [x_seq], [], y_out, 0)
        for b in seqs:
            x_grad, gain_b = row_call(ln_bwd_kernel, 32, b, [dhs[b]], [x_seq, y_grad], [gain], x_grad, 1)
            gain_part = gain_part + gain_b[0]
        gain_grad = lax.psum(gain_part, 'tp').astype(jnp.bfloat16)
        return y_out, x_grad, gain_grad, wqkv_grad, wout_grad

    specs_in = (P('dp', 'tp', None), P(None), P(None, 'tp', None), P('tp', None), P('dp', 'tp', None))
    specs_out = (P('dp', 'tp', None), P('dp', 'tp', None), P('dp'), P('dp', 'tp', None), P(('dp', 'tp'), None))
    return jax.shard_map(device_step, mesh=mesh, in_specs=specs_in, out_specs=specs_out, check_vma=False)
```

```python
import functools
import jax
import jax.numpy as jnp
from jax import lax
from jax.experimental import pallas as pl
from jax.experimental.pallas import tpu as pltpu
from jax.sharding import PartitionSpec as P

CLIP_QKV = 8.0
ROPE_THETA = 500000.0
LN_EPS = 1e-5
LOG2E = 1.4426950408889634
QBLK = 256
NT = (((1,), (1,)), ((), ()))
NN = (((1,), (0,)), ((), ()))
TN = (((0,), (0,)), ((), ()))


def dot32(a, b, dims):
    return lax.dot_general(a, b, dims, preferred_element_type=jnp.float32)


def ln_stats(x):
    row_mean = jnp.mean(x, axis=-1, keepdims=True)
    centered = x - row_mean
    variance = jnp.mean(centered * centered, axis=-1, keepdims=True)
    rstd = lax.rsqrt(variance + LN_EPS)
    return centered * rstd, rstd


def ln_fwd_kernel(x_ref, gain_ref, h_ref):
    normed, _ = ln_stats(x_ref[0].astype(jnp.float32))
    h_ref[...] = (normed * gain_ref[...].astype(jnp.float32)).astype(jnp.bfloat16)


def ln_bwd_kernel(dh_ref, x_ref, dy_ref, gain_ref, *refs):
    dx_ref, dgain_ref = refs[-2:]
    normed, rstd = ln_stats(x_ref[0].astype(jnp.float32))
    d_h = dh_ref[...].astype(jnp.float32)
    d_gain = jnp.sum(d_h * normed, axis=0, keepdims=True)
    d_normed = d_h * gain_ref[...].astype(jnp.float32)
    shift = jnp.mean(d_normed, axis=-1, keepdims=True)
    slope = jnp.mean(d_normed * normed, axis=-1, keepdims=True)
    d_x = rstd * (d_normed - shift - normed * slope)
    dx_ref[0] = (dy_ref[0].astype(jnp.float32) + d_x).astype(jnp.bfloat16)

    @pl.when(pl.program_id(0) == 0)
    def _():
        dgain_ref[...] = d_gain

    @pl.when(pl.program_id(0) > 0)
    def _():
        dgain_ref[...] += d_gain


def residual_kernel(o_ref, x_ref, *refs):
    y_ref = refs[-1]
    y_ref[0] = (x_ref[0].astype(jnp.float32) + o_ref[...].astype(jnp.float32)).astype(jnp.bfloat16)


def rope_tables(seq_len, head_dim):
    inv_freq = 1.0 / (ROPE_THETA ** (jnp.arange(0, head_dim, 2, dtype=jnp.float32) / head_dim))
    angles = jnp.arange(seq_len, dtype=jnp.float32)[:, None] * inv_freq[None, :]
    cos_t, sin_t = jnp.cos(angles), jnp.sin(angles)
    return jnp.concatenate([cos_t, cos_t], axis=-1), jnp.concatenate([-sin_t, sin_t], axis=-1)


def clip(v):
    return jnp.minimum(jnp.maximum(v, -CLIP_QKV), CLIP_QKV)


def rope(v_f32, cos_t, sin_t):
    return v_f32 * cos_t + pltpu.roll(v_f32, v_f32.shape[-1] // 2, 1) * sin_t


def unrope(v_f32, cos_t, sin_t):
    return v_f32 * cos_t - pltpu.roll(v_f32, v_f32.shape[-1] // 2, 1) * sin_t


def masked_tail(s, fill):
    top, tail = s[:-QBLK], s[-QBLK:]
    rows = lax.broadcasted_iota(jnp.int32, tail.shape, 0)
    cols = lax.broadcasted_iota(jnp.int32, tail.shape, 1)
    tail = jnp.where(rows <= cols, tail, fill)
    return tail if s.shape[0] == QBLK else jnp.concatenate([top, tail], axis=0)


def half_rows(chip_ref, seq):
    half = seq // 2
    own = pl.multiple_of(chip_ref[0] * half, half)
    return half, pl.ds(own, half), pl.ds(half - own, half)


def join(chip_ref, own_ref, oth_ref, dst):
    _, own, oth = half_rows(chip_ref, dst.shape[0])
    dst[own, :] = own_ref[...].reshape(own_ref.shape[-2:])
    dst[oth, :] = oth_ref[...].reshape(oth_ref.shape[-2:])


def split(chip_ref, src, dst_ref):
    half, own, oth = half_rows(chip_ref, src.shape[-2])
    at = (0,) * (len(src.shape) - 2)
    dst_ref[at + (slice(0, half),)] = src[at + (own,)]
    dst_ref[at + (slice(half, 2 * half),)] = src[at + (oth,)]


def attn_fwd_kernel(groups, dim, chip_ref, own_ref, oth_ref, cos_ref, sin_ref, out_ref, perm_ref, lse_ref,
                    qkv_scr, k_scr, vt_scr):
    head = pl.program_id(1)
    seq = qkv_scr.shape[0]

    @pl.when(head == 0)
    def _():
        join(chip_ref, own_ref, oth_ref, qkv_scr)
        k_in = clip(qkv_scr[:, groups * dim:(groups + 1) * dim].astype(jnp.float32))
        k_scr[...] = rope(k_in, cos_ref[...], sin_ref[...]).astype(jnp.bfloat16)
        v_in = clip(qkv_scr[:, (groups + 1) * dim:(groups + 2) * dim].astype(jnp.float32))
        vt_scr[...] = v_in.T.astype(jnp.bfloat16)

    col = pl.ds(pl.multiple_of(head * dim, dim), dim)
    scale = LOG2E * dim ** -0.5

    def scores(i):
        rows = slice(i * QBLK, (i + 1) * QBLK)
        q_in = clip(qkv_scr[rows, col].astype(jnp.float32))
        q_rot = rope(q_in, cos_ref[rows, :], sin_ref[rows, :]).astype(jnp.bfloat16)
        return dot32(k_scr[:(i + 1) * QBLK, :], q_rot, NT)

    blocks = seq // QBLK
    ahead = scores(0)
    for i in range(blocks):
        rows = slice(i * QBLK, (i + 1) * QBLK)
        s = masked_tail(ahead * scale, -1e30)
        if i + 1 < blocks:
            ahead = scores(i + 1)
        top = jnp.max(s, axis=0, keepdims=True)
        e = jnp.exp2(s - top)
        total = jnp.sum(e, axis=0, keepdims=True)
        prob = (e * (1.0 / total)).astype(jnp.bfloat16)
        o_t = dot32(vt_scr[:, :(i + 1) * QBLK], prob, NN)
        out_ref[rows, col] = o_t.T.astype(jnp.bfloat16)
        lse_ref[0, pl.ds(head, 1), rows] = top + jnp.log2(total)

    @pl.when(head == groups - 1)
    def _():
        split(chip_ref, out_ref, perm_ref)


def attn_bwd_kernel(groups, dim, chip_ref, own_ref, oth_ref, do_own_ref, do_oth_ref, lse_ref, cos_ref, sin_ref,
                    dqkv_ref, perm_ref, qkv_scr, do_scr, k_scr, kt_scr, v_scr, dk_scr, dv_scr):
    head = pl.program_id(1)
    seq = qkv_scr.shape[0]
    kcol = slice(groups * dim, (groups + 1) * dim)
    vcol = slice((groups + 1) * dim, (groups + 2) * dim)

    @pl.when(head == 0)
    def _():
        join(chip_ref, own_ref, oth_ref, qkv_scr)
        join(chip_ref, do_own_ref, do_oth_ref, do_scr)
        k_in = clip(qkv_scr[:, kcol].astype(jnp.float32))
        k_rot = rope(k_in, cos_ref[...], sin_ref[...])
        k_scr[...] = k_rot.astype(jnp.bfloat16)
        kt_scr[...] = k_rot.T.astype(jnp.bfloat16)
        v_scr[...] = clip(qkv_scr[:, vcol].astype(jnp.float32)).astype(jnp.bfloat16)
        dk_scr[...] = jnp.zeros_like(dk_scr)
        dv_scr[...] = jnp.zeros_like(dv_scr)

    col = pl.ds(pl.multiple_of(head * dim, dim), dim)
    scale = dim ** -0.5
    blocks = seq // QBLK

    def load(i):
        rows = slice(i * QBLK, (i + 1) * QBLK)
        kend = (i + 1) * QBLK
        q_raw = qkv_scr[rows, col].astype(jnp.float32)
        q_rot = rope(clip(q_raw), cos_ref[rows, :], sin_ref[rows, :]).astype(jnp.bfloat16)
        s = dot32(k_scr[:kend, :], q_rot, NT)
        dp = dot32(v_scr[:kend, :], do_scr[rows, col], NT)
        return rows, kend, q_raw, q_rot, s, dp

    ahead = load(0)
    for i in range(blocks):
        rows, kend, q_raw, q_rot, s, dp = ahead
        d_o = do_scr[rows, col]
        if i + 1 < blocks:
            ahead = load(i + 1)
        s = s * (LOG2E * scale) - lse_ref[0, pl.ds(head, 1), rows]
        p = jnp.exp2(masked_tail(s, -1e30))
        dv_scr[:kend, :] += dot32(p.astype(jnp.bfloat16), d_o, NN)
        dp = dp.astype(jnp.bfloat16).astype(jnp.float32)
        t = p * dp
        delta = jnp.sum(t, axis=0, keepdims=True)
        ds = (t - p * delta).astype(jnp.bfloat16)
        dk_scr[:kend, :] += dot32(ds, q_rot, NN)
        dq = (dot32(kt_scr[:, :kend], ds, NN) * scale).T.astype(jnp.bfloat16).astype(jnp.float32)
        dq = unrope(dq, cos_ref[rows, :], sin_ref[rows, :])
        dqkv_ref[0, rows, col] = jnp.where(jnp.abs(q_raw) < CLIP_QKV, dq, 0.0).astype(jnp.bfloat16)

    @pl.when(head == groups - 1)
    def _():
        k_raw = qkv_scr[:, kcol].astype(jnp.float32)
        v_raw = qkv_scr[:, vcol].astype(jnp.float32)
        dk = (dk_scr[...] * scale).astype(jnp.bfloat16).astype(jnp.float32)
        dk = unrope(dk, cos_ref[...], sin_ref[...])
        dqkv_ref[0, :, kcol] = jnp.where(jnp.abs(k_raw) < CLIP_QKV, dk, 0.0).astype(jnp.bfloat16)
        dqkv_ref[0, :, vcol] = jnp.where(jnp.abs(v_raw) < CLIP_QKV, dv_scr[...], 0.0).astype(jnp.bfloat16)
        split(chip_ref, dqkv_ref, perm_ref)


VMEM_MAX = 63 * 2 ** 20


def attn_params(kv_loc, groups, seq, dim, dots):
    return dict(
        compiler_params=pltpu.CompilerParams(dimension_semantics=("arbitrary", "arbitrary"),
                                             vmem_limit_bytes=VMEM_MAX),
        cost_estimate=pl.CostEstimate(flops=dots * 2 * kv_loc * groups * seq * seq * dim,
                                      bytes_accessed=2 * kv_loc * seq * dim * (2 * groups + 2) * 2,
                                      transcendentals=kv_loc * groups * seq * seq // 2))


def attn_fwd(chip, own, oth, cos_t, sin_t, dim):
    kv_loc, half, width = own.shape
    seq = 2 * half
    groups = width // dim - 2
    table = pl.BlockSpec((seq, dim), lambda n, h: (0, 0))
    piece = pl.BlockSpec((1, half, width), lambda n, h: (n, 0, 0))
    heads = pl.BlockSpec((seq, groups * dim), lambda n, h: (0, n))
    heads_shape = jax.ShapeDtypeStruct((seq, kv_loc * groups * dim), jnp.bfloat16)
    return pl.pallas_call(
        functools.partial(attn_fwd_kernel, groups, dim),
        grid=(kv_loc, groups),
        in_specs=[pl.BlockSpec(memory_space=pltpu.SMEM), piece, piece, table, table],
        out_specs=[heads, heads, pl.BlockSpec((1, groups, seq), lambda n, h: (n, 0, 0))],
        out_shape=[heads_shape, heads_shape, jax.ShapeDtypeStruct((kv_loc, groups, seq), jnp.float32)],
        scratch_shapes=[pltpu.VMEM((seq, width), jnp.bfloat16), pltpu.VMEM((seq, dim), jnp.bfloat16),
                        pltpu.VMEM((dim, seq), jnp.bfloat16)],
        name="attn_fwd",
        **attn_params(kv_loc, groups, seq, dim, 4),
    )(chip, own, oth, cos_t, sin_t)


def attn_bwd(chip, own, oth, do_own, do_oth, lse, cos_t, sin_t, dim):
    kv_loc, half, width = own.shape
    seq = 2 * half
    groups = width // dim - 2
    table = pl.BlockSpec((seq, dim), lambda n, h: (0, 0))
    piece = pl.BlockSpec((1, half, width), lambda n, h: (n, 0, 0))
    d_piece = pl.BlockSpec((half, groups * dim), lambda n, h: (0, n))
    wide = pl.BlockSpec((1, seq, width), lambda n, h: (n, 0, 0))
    wide_shape = jax.ShapeDtypeStruct((kv_loc, seq, width), jnp.bfloat16)
    return pl.pallas_call(
        functools.partial(attn_bwd_kernel, groups, dim),
        grid=(kv_loc, groups),
        in_specs=[pl.BlockSpec(memory_space=pltpu.SMEM), piece, piece, d_piece, d_piece,
                  pl.BlockSpec((1, groups, seq), lambda n, h: (n, 0, 0)), table, table],
        out_specs=[wide, wide],
        out_shape=[wide_shape, wide_shape],
        scratch_shapes=[pltpu.VMEM((seq, width), jnp.bfloat16), pltpu.VMEM((seq, groups * dim), jnp.bfloat16),
                        pltpu.VMEM((seq, dim), jnp.bfloat16), pltpu.VMEM((dim, seq), jnp.bfloat16),
                        pltpu.VMEM((seq, dim), jnp.bfloat16), pltpu.VMEM((seq, dim), jnp.float32),
                        pltpu.VMEM((seq, dim), jnp.float32)],
        name="attn_bwd",
        **attn_params(kv_loc, groups, seq, dim, 8),
    )(chip, own, oth, do_own, do_oth, lse, cos_t, sin_t)


def wqkv_grad_kernel(pieces, *refs):
    h_refs, d_refs, out_ref = refs[:pieces], refs[pieces:-1], refs[-1]
    half = h_refs[0].shape[0]
    for n in range(out_ref.shape[1]):
        total = 0.0
        for j in range(pieces):
            at = half * (j % 2)
            total += dot32(h_refs[j][...], d_refs[j // 2][n, at:at + half, :], TN)
        out_ref[:, n, :] = total.astype(jnp.bfloat16)


def wqkv_grad_call(h_pieces, d_qkv):
    half, rows = h_pieces[0].shape
    kv_loc, seq, width = d_qkv[0].shape
    block = 256
    return pl.pallas_call(
        functools.partial(wqkv_grad_kernel, len(h_pieces)), grid=(rows // block,),
        in_specs=[pl.BlockSpec((half, block), lambda r: (0, r))] * len(h_pieces)
        + [pl.BlockSpec((kv_loc, seq, width), lambda r: (0, 0, 0))] * len(d_qkv),
        out_specs=pl.BlockSpec((block, kv_loc, width), lambda r: (r, 0, 0)),
        out_shape=jax.ShapeDtypeStruct((rows, kv_loc, width), jnp.bfloat16),
        compiler_params=pltpu.CompilerParams(dimension_semantics=("arbitrary",), vmem_limit_bytes=VMEM_MAX),
        cost_estimate=pl.CostEstimate(flops=2 * half * len(h_pieces) * rows * kv_loc * width,
                                      bytes_accessed=4 * rows * kv_loc * width, transcendentals=0),
        name="wqkv_grad",
    )(*h_pieces, *d_qkv)


def row_call(body, rows, b, flat_in, full_in, extra_in, prev, extra_out):
    tokens, width = full_in[0].shape[1:]
    flat = pl.BlockSpec((rows, width), lambda r: (r, 0))
    full = pl.BlockSpec((1, rows, width), lambda r: (b, r, 0))
    wide = pl.BlockSpec((1, width), lambda r: (0, 0))
    args = [*flat_in, *full_in, *extra_in] + ([] if prev is None else [prev])
    specs = [flat] * len(flat_in) + [full] * len(full_in) + [wide] * len(extra_in)
    if prev is not None:
        specs.append(pl.BlockSpec(memory_space=pl.ANY))
    out_spec = flat if prev is None and not flat_in else full
    out_shape = (tokens, width) if prev is None and not flat_in else full_in[0].shape
    out_shape = [jax.ShapeDtypeStruct(out_shape, jnp.bfloat16)]
    out_shape += [jax.ShapeDtypeStruct((1, width), jnp.float32)] * extra_out
    return pl.pallas_call(
        body, grid=(tokens // rows,), in_specs=specs, out_specs=[out_spec] + [wide] * extra_out, out_shape=out_shape,
        input_output_aliases={} if prev is None else {len(args) - 1: 0},
        compiler_params=pltpu.CompilerParams(dimension_semantics=("arbitrary",), vmem_limit_bytes=VMEM_MAX),
        cost_estimate=pl.CostEstimate(flops=40 * tokens * width, bytes_accessed=2 * len(args) * tokens * width,
                                      transcendentals=0),
    )(*args)


def ein(spec, a, b):
    return jnp.einsum(spec, a, b, preferred_element_type=jnp.float32).astype(jnp.bfloat16)


def solution(mesh):
    def device_step(x_seq, ln_gain, w_qkv, w_out, y_grad):
        batch = x_seq.shape[0]
        kv_loc = w_qkv.shape[1]
        dim = (w_qkv.shape[2] - w_out.shape[0] // kv_loc) // 2
        gain = ln_gain.reshape(1, -1)
        cos_t, sin_t = rope_tables(x_seq.shape[1] * lax.axis_size('tp'), dim)
        chip = (lax.axis_index('tp') // 2).astype(jnp.int32).reshape(1)

        def across(v):
            return lax.ppermute(v, 'tp', [(d, (d + 2) % 4) for d in range(4)])

        def pair(v):
            return lax.all_gather(v, 'tp', axis=0, tiled=True, axis_index_groups=[[0, 1], [2, 3]])

        def scatter(v):
            return lax.psum_scatter(v, 'tp', scatter_dimension=0, tiled=True)

        seqs = range(batch)
        h_loc = [row_call(ln_fwd_kernel, 32, b, [], [x_seq], [gain], None, 0)[0] for b in seqs]
        g_loc = [y_grad[b] for b in seqs]
        h_far = [across(h_loc[b]) for b in seqs]
        g_far = [across(g_loc[b]) for b in seqs]
        h_own = [pair(h_loc[b]) for b in seqs]
        g_own = [pair(g_loc[b]) for b in seqs]
        h_oth = [pair(h_far[b]) for b in seqs]
        g_oth = [pair(g_far[b]) for b in seqs]
        qkv_own = [ein('sd,dnc->nsc', h_own[b], w_qkv) for b in seqs]
        d_own = [ein('sd,kd->sk', g_own[b], w_out) for b in seqs]
        qkv_oth, attn_perm, lse, outs, d_perm, dhs = [], [], [], [], [], []
        for b in seqs:
            qkv_oth.append(ein('sd,dnc->nsc', h_oth[b], w_qkv))
            a_seq, a_perm, lse_b = attn_fwd(chip, qkv_own[b], qkv_oth[b], cos_t, sin_t, dim)
            attn_perm.append(a_perm)
            lse.append(lse_b)
            outs.append(scatter(ein('sk,kd->sd', a_seq, w_out)))
        for b in seqs:
            d_oth = ein('sd,kd->sk', g_oth[b], w_out)
            d_seq, d_perm_b = attn_bwd(chip, qkv_own[b], qkv_oth[b], d_own[b], d_oth, lse[b], cos_t, sin_t, dim)
            d_perm.append(d_perm_b)
            dhs.append(scatter(ein('nsc,dnc->sd', d_seq, w_qkv)))
        g_all = jnp.concatenate([v for b in seqs for v in (g_own[b], g_oth[b])], 0)
        wout_grad = ein('sk,sd->kd', jnp.concatenate(attn_perm, 0), g_all)
        wqkv_grad = wqkv_grad_call([v for b in seqs for v in (h_own[b], h_oth[b])], d_perm)
        y_out, x_grad, gain_part = None, None, 0.0
        for b in seqs:
            (y_out,) = row_call(residual_kernel, 64, b, [outs[b]], [x_seq], [], y_out, 0)
        for b in seqs:
            x_grad, gain_b = row_call(ln_bwd_kernel, 32, b, [dhs[b]], [x_seq, y_grad], [gain], x_grad, 1)
            gain_part = gain_part + gain_b[0]
        gain_grad = lax.psum(gain_part, 'tp').astype(jnp.bfloat16)
        return y_out, x_grad, gain_grad, wqkv_grad, wout_grad

    specs_in = (P('dp', 'tp', None), P(None), P(None, 'tp', None), P('tp', None), P('dp', 'tp', None))
    specs_out = (P('dp', 'tp', None), P('dp', 'tp', None), P('dp'), P('dp', 'tp', None), P(('dp', 'tp'), None))
    return jax.shard_map(device_step, mesh=mesh, in_specs=specs_in, out_specs=specs_out, check_vma=False)
```
